32 devices in a mesh: dp: 32 (over z, y, x, core).
Axes of the slice: x: 2, y: 2, z: 4, core: 2. Of those that a mesh axis runs over, the one named last changes fastest.
Arguments:
- points: float32 [16384, 17], P('dp')
- targets: float32 [16384], P('dp')
- probes: float32 [16384, 16], P('dp')
- log_l: float32 [], replicated
- log_s: float32 [], replicated
- log_sigma: float32 [], replicated
Outputs:
- output 1: float32 [16384], P('dp')
- output 2: float32 [16384, 16], P('dp')
- output 3: float32 [4], replicated
All inputs are finite; a program needn't handle non-finite values.
Results may differ from the reference program's by a relative error of at most 0.001.
Values sent between devices are 32-bit elements.
A program may use at most 1 GiB of HBM per device.

```python
import math
import jax
import jax.numpy as jnp
from jax import lax

N = 16384
D = 17
PROBES = 16
STEPS = 20
ROW_TILE = 64


def kernel_width(n_points, dimension):
    grid_size = 4000
    exponent = 0.5 * (dimension - 3)
    offsets = [2.0 * ((index + 0.5) / grid_size) ** 2 for index in range(grid_size)]
    weights = [4.0 * (index + 0.5) / grid_size ** 2 * (offset * (2.0 - offset)) ** exponent for index, offset in enumerate(offsets)]
    weight_total = sum(weights)
    target_mass = 16.0 / (n_points - 1)
    lower_log = math.log(1e-3)
    upper_log = math.log(1e7)
    for attempt in range(60):
        middle_log = 0.5 * (lower_log + upper_log)
        rate_value = math.exp(middle_log)
        kernel_mass = sum(weight * math.exp(-rate_value * offset) for offset, weight in zip(offsets, weights)) / weight_total
        lower_log, upper_log = (middle_log, upper_log) if kernel_mass > target_mass else (lower_log, middle_log)
    return dimension / math.exp(0.5 * (lower_log + upper_log))


def setup_inputs(seed: int = 0) -> dict:
    keys = jax.random.split(jax.random.key(seed), 7)
    gauss = jax.random.normal(keys[0], (N, D), jnp.float32)
    points = gauss * (math.sqrt(D) / jnp.linalg.norm(gauss, axis=1, keepdims=True))
    direction = jax.random.normal(keys[1], (D,), jnp.float32) / math.sqrt(D)
    targets = jnp.sin(jnp.dot(points, direction)) + 0.5 * jax.random.normal(keys[2], (N,), jnp.float32)
    probes = 2.0 * jax.random.bernoulli(keys[3], 0.5, (N, PROBES)).astype(jnp.float32) - 1.0
    base_log_l = 0.5 * math.log(kernel_width(N, D))
    log_l = base_log_l + 0.05 * jax.random.normal(keys[4], (), jnp.float32)
    log_s = 0.1 * jax.random.normal(keys[5], (), jnp.float32)
    log_sigma = math.log(0.25) + 0.1 * jax.random.normal(keys[6], (), jnp.float32)
    return {"points": points, "targets": targets, "probes": probes, "log_l": log_l, "log_s": log_s, "log_sigma": log_sigma}


def kernel_block(row_points, points, sq_norms, inv_two_l2):
    cross = jnp.einsum("id,kd->ik", row_points, points, precision=lax.Precision.HIGHEST)
    row_sq = jnp.sum(row_points * row_points, axis=1)
    dist_sq = jnp.maximum(row_sq[:, None] + sq_norms[None, :] - 2.0 * cross, 0.0)
    return jnp.exp(-dist_sq * inv_two_l2), dist_sq


def reference(points, targets, probes, log_l, log_s, log_sigma):
    inv_two_l2 = 0.5 * jnp.exp(-2.0 * log_l)
    out_var = jnp.exp(2.0 * log_s)
    noise_var = jnp.exp(2.0 * log_sigma)
    sq_norms = jnp.sum(points * points, axis=1)
    row_tiles = points.reshape(N // ROW_TILE, ROW_TILE, D)

    def apply_kernel(directions):
        def one_tile(row_points):
            kernel = kernel_block(row_points, points, sq_norms, inv_two_l2)[0]
            return jnp.dot(kernel, directions, precision=lax.Precision.HIGHEST, preferred_element_type=jnp.float32)
        product = lax.map(one_tile, row_tiles).reshape(N, PROBES + 1)
        return out_var * product + noise_var * directions

    right_sides = jnp.concatenate([targets[:, None], probes], axis=1)

    def cg_step(carry, step_input):
        solved, residual, search, res_norm = carry
        product = apply_kernel(search)
        alpha = res_norm / jnp.sum(search * product, axis=0)
        solved = solved + alpha * search
        residual = residual - alpha * product
        new_norm = jnp.sum(residual * residual, axis=0)
        search = residual + (new_norm / res_norm) * search
        return (solved, residual, search, new_norm), None

    start_state = (jnp.zeros_like(right_sides), right_sides, right_sides, jnp.sum(right_sides * right_sides, axis=0))
    final_state, unused = lax.scan(cg_step, start_state, None, length=STEPS)
    solved = final_state[0]
    u_solve = solved[:, 0]
    v_solve = solved[:, 1:]
    left = jnp.concatenate([u_solve[:, None], -v_solve / PROBES], axis=1)
    right = jnp.concatenate([u_solve[:, None], probes], axis=1)
    left_tiles = left.reshape(N // ROW_TILE, ROW_TILE, PROBES + 1)

    def grad_tile(tile):
        row_points, row_left = tile
        kernel, dist_sq = kernel_block(row_points, points, sq_norms, inv_two_l2)
        kern_right = jnp.dot(kernel, right, precision=lax.Precision.HIGHEST, preferred_element_type=jnp.float32)
        dist_right = jnp.dot(kernel * dist_sq, right, precision=lax.Precision.HIGHEST, preferred_element_type=jnp.float32)
        return jnp.stack([jnp.sum(row_left * dist_right), jnp.sum(row_left * kern_right)])

    sums = jnp.sum(lax.map(grad_tile, (row_tiles, left_tiles)), axis=0)
    hyper_grads = jnp.stack([
        out_var * inv_two_l2 * sums[0],
        out_var * sums[1],
        noise_var * jnp.sum(left * right),
        0.5 * jnp.sum(targets * u_solve),
    ]) / N
    return u_solve, v_solve, hyper_grads
```

```python
import functools
import math

import jax
import jax.numpy as jnp
from jax import lax
from jax.experimental import pallas as pl
from jax.experimental.pallas import tpu as pltpu
from jax.sharding import PartitionSpec as P

CG_STEPS = 20
NDEV = 32
ROWS = 512
GR = 24
NP = 16
KW = 256
KT = 1024
CH = 128
LOG2E = math.log2(math.e)
LN2 = math.log(2.0)
f32 = jnp.float32
bf16 = jnp.bfloat16
MESH = pl.DeviceIdType.MESH


def dot(a, b):
    return lax.dot_general(a, b, (((1,), (0,)), ((), ())), preferred_element_type=f32)


def parts(x):
    h = x.astype(bf16).astype(f32)
    r = x - h
    m = r.astype(bf16).astype(f32)
    return h, m, r - m


def kernel(pay_ref, scal_ref, sol_ref, hyp_ref,
           g0, gq, pall, rall, uall, xk, xi, pp, acc, qown, tsum, tall,
           ha, ma, la, hb, mb, lb, s_send, s_recv, i_send, i_recv, t_send, t_recv):
    me = lax.axis_index("dp")
    n_total = NDEV * ROWS
    out_var = scal_ref[0:1, 0:1]
    noise_var = scal_ref[1:2, 0:1]
    lane_scale = scal_ref[2:3, 0:1]
    row_id = lax.broadcasted_iota(jnp.int32, (GR, 1), 0)
    live = row_id < NP + 1

    def exchange(src, dst_of, send, recv):
        def start(d, c):
            to = lax.rem(me + d, NDEV)
            pltpu.make_async_remote_copy(src_ref=src, dst_ref=dst_of(me), send_sem=send.at[d],
                                         recv_sem=recv.at[me], device_id=(to,), device_id_type=MESH).start()
            return c
        lax.fori_loop(1, NDEV, start, 0)

        def finish(d, c):
            frm = lax.rem(me + NDEV - d, NDEV)
            cp = pltpu.make_async_remote_copy(src_ref=src, dst_ref=dst_of(frm), send_sem=send.at[d],
                                              recv_sem=recv.at[frm], device_id=(frm,), device_id_type=MESH)
            cp.wait_send()
            cp.wait_recv()
            return c
        lax.fori_loop(1, NDEV, finish, 0)

    g0[me] = pay_ref[...]
    exchange(pay_ref, lambda b: g0.at[b], i_send, i_recv)

    aug = pay_ref[0:GR, :]
    own_rows = lax.broadcasted_iota(jnp.int32, (GR, ROWS), 0)
    norm_row = pay_ref[17:18, :]
    side = jnp.where(own_rows < 17, aug * lane_scale, jnp.where(own_rows == 17, 1.0, jnp.where(own_rows == 18, norm_row, 0.0)))
    ih, im, il = parts(side)
    zpad = jnp.zeros((KW - 6 * GR, ROWS), f32)
    xi[...] = jnp.concatenate([ih, im, il, ih, im, ih, zpad], axis=0).astype(bf16)

    def prepare(b, rho):
        kh, km, kl = parts(g0[b, 0:GR, :])
        stacked = jnp.concatenate([kh, kh, kh, km, km, kl, zpad], axis=0)
        xk[pl.ds(pl.multiple_of(b * ROWS, ROWS), ROWS), :] = stacked.T.astype(bf16)
        right = g0[b, GR:2 * GR, :]
        pall[b] = right
        rall[b] = right
        uall[b] = jnp.zeros_like(right)
        put_parts(b, right)
        return rho + right * right

    def put_parts(b, x):
        h, m, l = parts(x)
        both = jnp.concatenate([m, h, l, jnp.zeros((8, ROWS), f32)], axis=0)
        pp[:, pl.ds(pl.multiple_of(b * ROWS, ROWS), ROWS)] = both.astype(bf16)

    zacc = jnp.zeros((GR, ROWS), f32)
    rho0 = jnp.sum(lax.fori_loop(0, NDEV, prepare, zacc), axis=1, keepdims=True)

    bufs = ((ha, ma, la), (hb, mb, lb))

    def product(with_dist):
        def gen(k0, b, c):
            hn, mn, ln = bufs[b]
            s = jnp.minimum(dot(xk[pl.ds(k0 + c, CH), :], xi[...]), 0.0)
            return s

        def put(s, b, c):
            hn, mn, ln = bufs[b]
            o = slice(c, c + CH)
            e = jnp.exp2(s)
            if with_dist:
                e = e * (-LN2 * s)
            hn[o, :] = e.astype(bf16)
            r = e - hn[o, :].astype(f32)
            mn[o, :] = r.astype(bf16)
            ln[o, :] = (r - mn[o, :].astype(f32)).astype(bf16)

        def half(k_new, b_new, k_old, b_old):
            h_, m_, l_ = bufs[b_old]
            a80 = a48 = a32 = None
            for c in range(0, KT, CH):
                o = slice(c, c + CH)
                s = gen(k_new, b_new, c)
                p = pp[:, pl.ds(k_old + c, CH)]
                x, y, z = dot(p, h_[o, :]), dot(p[0:48], m_[o, :]), dot(p[16:48], l_[o, :])
                a80, a48, a32 = (x, y, z) if a80 is None else (a80 + x, a48 + y, a32 + z)
                put(s, b_new, c)
            acc[...] += a80
            acc[0:48, :] += a48
            acc[16:48, :] += a32

        acc[...] = jnp.zeros_like(acc)
        for c in range(0, KT, CH):
            put(gen(0, 0, c), 0, c)

        def body(u, c):
            k = lambda n: pl.multiple_of(lax.rem(2 * u + n, n_total // KT) * KT, KT)
            half(k(1), 1, k(0), 0)
            half(k(2), 0, k(1), 1)
            return c
        lax.fori_loop(0, n_total // KT // 2, body, 0)
        return acc[0:24, :] + acc[24:48, :] + acc[48:72, :]

    def step(i, rho):
        slot = lax.rem(i, 2)
        qown[slot] = out_var * product(False) + noise_var * pall[me]
        gq[slot, me] = qown[slot]
        exchange(qown.at[slot], lambda b: gq.at[slot, b], s_send.at[slot], s_recv.at[slot])
        pq = lax.fori_loop(0, NDEV, lambda b, a: a + pall[b] * gq[slot, b], zacc)
        pq = jnp.sum(pq, axis=1, keepdims=True)
        alpha = jnp.where(live, rho / jnp.where(live, pq, 1.0), 0.0)

        def residual(b, a):
            r = rall[b] - alpha * gq[slot, b]
            rall[b] = r
            uall[b] = uall[b] + alpha * pall[b]
            return a + r * r
        new = jnp.sum(lax.fori_loop(0, NDEV, residual, zacc), axis=1, keepdims=True)
        beta = jnp.where(live, new / jnp.where(live, rho, 1.0), 0.0)

        def search(b, c):
            p = rall[b] + beta * pall[b]
            pall[b] = p
            put_parts(b, p)
            return c
        lax.fori_loop(0, NDEV, search, 0)
        return new
    lax.fori_loop(0, CG_STEPS, step, rho0)

    own_u = uall[me]
    sol_ref[...] = own_u
    is_y = row_id == NP

    def columns(b):
        return jnp.where(is_y, uall[b], g0[b, GR:2 * GR, :])

    def final_parts(b, c):
        put_parts(b, columns(b))
        return c
    lax.fori_loop(0, NDEV, final_parts, 0)
    left = jnp.where(is_y, own_u, own_u * (-1.0 / NP))
    right_own = columns(me)
    own_y = pay_ref[GR:2 * GR, :]
    dist_right = product(True)
    kern_right = product(False)

    def total(x):
        return jnp.sum(jnp.sum(x, axis=1, keepdims=True), axis=0, keepdims=True)
    g_l = out_var * total(left * dist_right)
    g_s = out_var * total(left * kern_right)
    g_n = noise_var * total(left * right_own)
    fit = 0.5 * total(jnp.where(is_y, own_y * own_u, 0.0))
    r8 = lax.broadcasted_iota(jnp.int32, (8, 128), 0)
    tile = jnp.where(r8 == 0, g_l, jnp.where(r8 == 1, g_s, jnp.where(r8 == 2, g_n, jnp.where(r8 == 3, fit, 0.0)))) / n_total
    tsum[...] = tile
    tall[me] = tile
    exchange(tsum, lambda b: tall.at[b], t_send, t_recv)
    hyp_ref[...] = lax.fori_loop(0, NDEV, lambda b, a: a + tall[b], jnp.zeros((8, 128), f32))


def solution(mesh):
    def local(points_own, targets_own, probes_own, log_l, log_s, log_sigma):
        inv_two_l2 = 0.5 * jnp.exp(-2.0 * log_l)
        rate = LOG2E * inv_two_l2
        scal = jnp.stack([jnp.exp(2.0 * log_s), jnp.exp(2.0 * log_sigma), 2.0 * rate])
        scal = jnp.broadcast_to(jnp.pad(scal, (0, 5))[:, None], (8, 128))
        norm = -rate * jnp.sum(points_own * points_own, axis=1)
        one = jnp.ones((1, ROWS), f32)
        pay = jnp.concatenate([points_own.T, norm[None, :], one, jnp.zeros((5, ROWS), f32),
                               probes_own.T, targets_own[None, :], jnp.zeros((7, ROWS), f32)], axis=0)
        dma = pltpu.SemaphoreType.DMA
        sol, hyp = pl.pallas_call(
            kernel,
            out_shape=(jax.ShapeDtypeStruct((GR, ROWS), f32), jax.ShapeDtypeStruct((8, 128), f32)),
            in_specs=[pl.BlockSpec(memory_space=pltpu.VMEM)] * 2,
            out_specs=(pl.BlockSpec(memory_space=pltpu.VMEM),) * 2,
            scratch_shapes=[
                pltpu.VMEM((NDEV, 2 * GR, ROWS), f32),
                pltpu.VMEM((2, NDEV, GR, ROWS), f32),
                pltpu.VMEM((NDEV, GR, ROWS), f32),
                pltpu.VMEM((NDEV, GR, ROWS), f32),
                pltpu.VMEM((NDEV, GR, ROWS), f32),
                pltpu.VMEM((NDEV * ROWS, KW), bf16),
                pltpu.VMEM((KW, ROWS), bf16),
                pltpu.VMEM((80, NDEV * ROWS), bf16),
                pltpu.VMEM((80, ROWS), f32),
                pltpu.VMEM((2, GR, ROWS), f32),
                pltpu.VMEM((8, 128), f32),
                pltpu.VMEM((NDEV, 8, 128), f32),
            ] + [pltpu.VMEM((KT, ROWS), bf16)] * 6 + [
                dma((2, NDEV)), dma((2, NDEV)), dma((NDEV,)), dma((NDEV,)), dma((NDEV,)), dma((NDEV,)),
            ],
            compiler_params=pltpu.CompilerParams(has_side_effects=True, vmem_limit_bytes=60 * 2**20),
            name="gp_cg",
        )(pay, scal)
        return sol[NP], sol[:NP].T, hyp[:4, 0]

    return jax.shard_map(
        local,
        mesh=mesh,
        in_specs=(P("dp", None), P("dp"), P("dp", None), P(), P(), P()),
        out_specs=(P("dp"), P("dp", None), P()),
        check_vma=False,
    )
```

```python
import math

import jax
import jax.numpy as jnp
import numpy as np
from jax import lax
from jax.experimental import pallas as pl
from jax.experimental.pallas import tpu as pltpu
from jax.sharding import PartitionSpec as P

CG_STEPS = 20
NDEV = 32
ROWS = 512
HALF = 256
NP = 16
DIM = 17
N = NDEV * ROWS
PRE = 12288
REST = N - PRE
LOG2E = math.log2(math.e)
LN2 = math.log(2.0)
f32 = jnp.float32
bf16 = jnp.bfloat16
MESH = pl.DeviceIdType.MESH

TERMS = ((0, 0), (0, 1), (0, 2), (1, 0), (1, 1), (2, 0))


def placements():
    col, row, right, left = (np.zeros((72, 128), np.float32) for _ in range(4))
    j = 0
    for a, b in TERMS:
        for d in range(DIM):
            col[24 * a + d, j] = row[24 * b + d, j] = 1.0
            j += 1
    for t in range(3):
        col[24 * t + 17, j] = row[18, j] = 1.0
        j += 1
    for t in range(3):
        col[18, j] = row[24 * t + 17, j] = 1.0
        j += 1
    j = 0
    for t in range(3):
        for d in range(NP):
            right[d, j] = left[24 * t + d, j] = 1.0
            j += 1
    for a, b in TERMS:
        right[24 * a + NP, j] = left[24 * b + NP, j] = 1.0
        j += 1
    return np.stack([col, row, right, left])


def dot(a, b):
    return lax.dot_general(a, b, (((1,), (0,)), ((), ())), preferred_element_type=f32)


def dot_t(a, b):
    return lax.dot_general(a, b, (((0,), (0,)), ((), ())), preferred_element_type=f32)


def parts(x):
    h = x.astype(bf16).astype(f32)
    r = x - h
    m = r.astype(bf16).astype(f32)
    return h, m, r - m


def wide(v):
    first = lax.broadcasted_iota(jnp.int32, (8, 128), 0) == 0
    y0 = jnp.where(first, v[4], 0.0)
    y1 = jnp.where(first, pltpu.roll(v[4], 7, 0), 0.0)
    top = jnp.concatenate([v[0], v[2], y0], axis=0)
    return jnp.concatenate([top, jnp.concatenate([v[1], v[3], y1], axis=0)], axis=1)


def narrow(q):
    row = lax.broadcasted_iota(jnp.int32, (8, 128), 0)
    y0, y1 = q[16:24, 0:128], q[16:24, 128:256]
    y = jnp.where(row == 0, y0, jnp.where(row == 1, pltpu.roll(y1, 1, 0), 0.0))
    return jnp.stack([q[0:8, 0:128], q[0:8, 128:256], q[8:16, 0:128], q[8:16, 128:256], y])


def kernel(pay_ref, scal_ref, place_ref, sol_ref, hyp_ref,
           gq, zall, pall, rall, uall, xk, xi, pp, acc, qown, tsum, tall,
           ph, pm, pl_, rh, rm, rl, send, recv, t_send, t_recv):
    me = lax.axis_index("dp")
    sib = me + 1 - 2 * lax.rem(me, 2)
    out_var = scal_ref[0:1, 0:1]
    noise_var = scal_ref[1:2, 0:1]
    rate = scal_ref[2:3, 0:1]

    def flip(i, bit):
        return i + bit - 2 * bit * lax.rem(i // bit, 2)

    def shift_z(i, k):
        return lax.rem(i // 8 + k, 4) * 8 + lax.rem(i, 8)

    nbrs = (flip(me, 2), flip(me, 4), flip(flip(me, 2), 4))

    class Gather:
        def __init__(self, slot, h, src, into=None):
            self.slot, self.h, self.src, self.k = slot, h, src, 0
            self.into = into or (lambda block: gq.at[slot, h, block])

        def copy(self, block, src, to, k):
            return pltpu.make_async_remote_copy(
                src_ref=src, dst_ref=self.into(block), send_sem=send.at[self.h, k],
                recv_sem=recv.at[self.slot, self.h, block], device_id=(to,), device_id_type=MESH)

        def put(self, block, src, to):
            self.copy(block, src, to, self.k).start()
            self.k += 1

        def arrived(self, block):
            self.copy(block, self.src, sib, 0).wait_recv()
            return self.into(block)

        def own(self):
            for dz in (1, 3, 2):
                self.put(me, self.src, shift_z(me, dz))
            for t in nbrs:
                self.put(me, self.src, t)
            self.put(me, self.src, sib)

        def lines(self):
            for dz in (1, 3, 2):
                b = shift_z(me, dz)
                src = self.arrived(b)
                for t in nbrs:
                    self.put(b, src, t)
                self.put(b, src, sib)

        def planes(self):
            for dz in (0, 1, 3, 2):
                for t in nbrs:
                    b = shift_z(t, dz)
                    self.put(b, self.arrived(b), sib)

        def finish(self):
            def wait_in(d, c):
                self.arrived(lax.rem(sib + 2 * d, NDEV))
                return c
            lax.fori_loop(0, NDEV // 2, wait_in, 0)

            def wait_out(k, c):
                self.copy(me, self.src, sib, k).wait_send()
                return c
            lax.fori_loop(0, self.k, wait_out, 0)

    def split_to(e, hr, mr, lr, idx):
        hr[idx] = e.astype(bf16)
        r = e - hr[idx].astype(f32)
        mr[idx] = r.astype(bf16)
        lr[idx] = (r - mr[idx].astype(f32)).astype(bf16)

    def ahead(k0, rows, chunk=256, sub=64):
        for c in range(0, rows, chunk):
            s = dot(xk[pl.ds(k0 + c, chunk), :], xi[...])
            for r in range(0, chunk, sub):
                for h in (0, 1):
                    e = jnp.exp2(jnp.minimum(s[r:r + sub, h * HALF:(h + 1) * HALF], 0.0))
                    split_to(e, ph, pm, pl_, (h, pl.ds(k0 + c + r, sub), slice(None)))

    def apply(h, k0, rows, bufs):
        p = jnp.concatenate([pp[:, pl.ds(k0, rows)], jnp.zeros((48, rows), bf16)], axis=0)
        a = dot(p, bufs[0]) + dot(p, bufs[1]) + dot(p, bufs[2])
        return a[0:72]

    TILE, NEW = 3072, 1024

    def half_product(h):
        acc[...] = jnp.zeros_like(acc)
        lanes = pl.ds(h * HALF, HALF)

        def body(i, c):
            k0 = pl.multiple_of(i * TILE, TILE)
            n0 = pl.multiple_of(i * NEW, NEW)
            total = None
            for j in range(4):
                s = dot(xk[pl.ds(PRE + n0 + j * 256, 256), :], xi[:, lanes])
                kk, w = k0 + j * (TILE // 4), TILE // 4
                a = apply(h, kk, w, [ref[h, pl.ds(kk, w), :] for ref in (ph, pm, pl_)])
                total = a if total is None else total + a
                for r in range(0, 256, 64):
                    e = jnp.exp2(jnp.minimum(s[r:r + 64, :], 0.0))
                    split_to(e, rh, rm, rl, (pl.ds(n0 + j * 256 + r, 64), slice(None)))
            acc[...] += total
            return c
        lax.fori_loop(0, PRE // TILE, body, 0)
        a = apply(h, PRE, REST, [ref[...] for ref in (rh, rm, rl)]) + acc[...]
        return a[0:24] + a[24:48] + a[48:72]

    for h in (0, 1):
        uall[me, h] = pay_ref[0, h]
        gq[1, h, me] = pay_ref[1, h]
    xs = [Gather(0, h, pay_ref.at[0, h], lambda b, h=h: uall.at[b, h]) for h in (0, 1)]
    for g in xs:
        g.own()
    for g in xs:
        g.lines()
    for g in xs:
        g.planes()
    for g in xs:
        g.finish()
    row24 = lax.broadcasted_iota(jnp.int32, (24, HALF), 0)

    def augmented(v, scale):
        w = wide(v)
        norm = -rate * jnp.sum(w * w, axis=0, keepdims=True)
        return jnp.where(row24 == 17, norm, jnp.where(row24 == 18, 1.0, w * scale))

    def stack(x):
        return jnp.concatenate(parts(x), axis=0).astype(bf16)

    for h in (0, 1):
        side = stack(augmented(pay_ref[0, h], 2.0 * rate))
        xi[:, h * HALF:(h + 1) * HALF] = dot_t(place_ref[1], side).astype(bf16)

    def pack_points(b, c):
        for h in (0, 1):
            x = stack(augmented(uall[b, h], 1.0))
            xk[pl.ds(pl.multiple_of(b * ROWS + h * HALF, HALF), HALF), :] = dot_t(x, place_ref[0]).astype(bf16)
        return c

    bs = [Gather(1, h, pay_ref.at[1, h]) for h in (0, 1)]
    for g in bs:
        g.own()
    lax.fori_loop(0, NDEV, pack_points, 0)
    AHEAD = 2048

    def ahead_loop(lo, hi):
        def body(i, c):
            ahead(pl.multiple_of(i * AHEAD, AHEAD), AHEAD)
            return c
        lax.fori_loop(lo, hi, body, 0)

    for g in bs:
        g.lines()
    ahead_loop(0, 3)
    for g in bs:
        g.planes()
    ahead_loop(3, 6)
    for g in bs:
        g.finish()

    def put_parts(b, h, v):
        a, m, l = parts(wide(v))
        both = jnp.concatenate([m, a, l, jnp.zeros((8, HALF), f32)], axis=0)
        pp[:, pl.ds(pl.multiple_of(b * ROWS + h * HALF, HALF), HALF)] = both.astype(bf16)

    zero5 = jnp.zeros((5, 8, 128), f32)

    def column_sums(x):
        both = jnp.concatenate([x[0] + x[1], x[2] + x[3], x[4]], axis=0)
        s = jnp.sum(both, axis=1, keepdims=True)
        return s[0:8], s[8:16], s[16:17] + s[17:18]

    def spread(s):
        a, b, y = (jnp.broadcast_to(x, (8, 128)) for x in s)
        return jnp.stack([a, a, b, b, y])

    def begin(b, a):
        for h in (0, 1):
            v = gq[1, h, b]
            zall[b, h] = v
            pall[b, h] = v
            rall[b, h] = v
            uall[b, h] = jnp.zeros_like(v)
            put_parts(b, h, v)
            a = a + v * v
        return a
    rho0 = column_sums(lax.fori_loop(0, NDEV, begin, zero5))

    def step(i, rho):
        slot = lax.rem(i, 2)
        gs = []
        for h in (0, 1):
            q = narrow(half_product(h))
            qown[slot, h] = out_var * q + noise_var * pall[me, h]
            gq[slot, h, me] = qown[slot, h]
            g = Gather(slot, h, qown.at[slot, h])
            g.own()
            gs.append(g)
        gs[0].lines()
        ahead_loop(0, 3)
        gs[0].planes()
        gs[1].lines()
        ahead_loop(3, 6)
        gs[1].planes()
        gs[0].finish()
        gs[1].finish()

        def inner(b, a):
            for h in (0, 1):
                a = a + pall[b, h] * gq[slot, h, b]
            return a
        pq = column_sums(lax.fori_loop(0, NDEV, inner, zero5))
        alpha = spread([r / q for r, q in zip(rho, pq)])

        def residual(b, a):
            for h in (0, 1):
                r = rall[b, h] - alpha * gq[slot, h, b]
                rall[b, h] = r
                uall[b, h] = uall[b, h] + alpha * pall[b, h]
                a = a + r * r
            return a
        new = column_sums(lax.fori_loop(0, NDEV, residual, zero5))
        beta = spread([n / r for n, r in zip(new, rho)])

        def search(b, c):
            for h in (0, 1):
                p = rall[b, h] + beta * pall[b, h]
                pall[b, h] = p
                put_parts(b, h, p)
            return c
        lax.fori_loop(0, NDEV, search, 0)
        return new
    lax.fori_loop(0, CG_STEPS, step, rho0)

    ids = lax.broadcasted_iota(jnp.int32, (5, 8, 128), 0)
    is_y = ids == 4
    own_sum = jnp.zeros((5, 8, 128), f32)
    fit_sum = jnp.zeros((5, 8, 128), f32)
    for h in (0, 1):
        u = uall[me, h]
        z = zall[me, h]
        sol_ref[h] = u
        left = jnp.where(is_y, u, u * (-1.0 / NP))
        own_sum = own_sum + left * jnp.where(is_y, u, z)
        fit_sum = fit_sum + jnp.where(is_y, u * z, 0.0)
        pp[:, h * HALF:(h + 1) * HALF] = jnp.zeros((80, HALF), bf16)
        ai = dot_t(place_ref[3], stack(wide(left))).astype(bf16)
        pp[0:64, h * HALF:(h + 1) * HALF] = ai[0:64]

    def pair_sums(b, carry):
        a_s, a_l = carry
        for h in (0, 1):
            right = jnp.where(is_y, uall[b, h], zall[b, h])
            ck = dot_t(stack(wide(right)), place_ref[2]).astype(bf16)
            k0 = pl.multiple_of(b * ROWS + h * HALF, HALF)
            s = dot(xk[pl.ds(k0, HALF), :], xi[...])
            g = dot(ck[:, 0:64], pp[0:64, 0:ROWS])
            for r in range(0, HALF, 8):
                sr = jnp.minimum(s[r:r + 8], 0.0)
                t = jnp.exp2(sr) * g[r:r + 8]
                a_s = a_s + t
                a_l = a_l + t * sr
        return a_s, a_l
    zrow = jnp.zeros((8, ROWS), f32)
    a_s, a_l = lax.fori_loop(0, NDEV, pair_sums, (zrow, zrow))

    def total(x):
        return jnp.sum(jnp.sum(x, axis=1, keepdims=True), axis=0, keepdims=True)

    def total5(x):
        return total(x[0] + x[1] + x[2] + x[3] + x[4])
    g_l = out_var * (-LN2) * total(a_l)
    g_s = out_var * total(a_s)
    g_n = noise_var * total5(own_sum)
    fit = 0.5 * total5(fit_sum)
    r8 = lax.broadcasted_iota(jnp.int32, (8, 128), 0)
    tile = jnp.where(r8 == 0, g_l, jnp.where(r8 == 1, g_s, jnp.where(r8 == 2, g_n, jnp.where(r8 == 3, fit, 0.0)))) / N
    tsum[...] = tile
    tall[me] = tile

    def t_copy(to, block, k):
        return pltpu.make_async_remote_copy(src_ref=tsum, dst_ref=tall.at[block], send_sem=t_send.at[k],
                                            recv_sem=t_recv.at[block], device_id=(to,), device_id_type=MESH)

    def t_start(d, c):
        t_copy(lax.rem(me + d, NDEV), me, d).start()
        return c
    lax.fori_loop(1, NDEV, t_start, 0)

    def t_finish(d, c):
        cp = t_copy(sib, lax.rem(me + d, NDEV), d)
        cp.wait_send()
        cp.wait_recv()
        return c
    lax.fori_loop(1, NDEV, t_finish, 0)
    hyp_ref[...] = lax.fori_loop(0, NDEV, lambda b, a: a + tall[b], jnp.zeros((8, 128), f32))


def to_half_blocks(main, last):
    m = main.reshape(2, 8, 2, 2, 128).transpose(2, 0, 3, 1, 4).reshape(2, 4, 8, 128)
    y = jnp.pad(last.reshape(2, 1, 2, 128), ((0, 0), (0, 0), (0, 6), (0, 0)))
    return jnp.concatenate([m, y], axis=1)


def solution(mesh):
    def local(points_own, targets_own, probes_own, log_l, log_s, log_sigma):
        rate = LOG2E * 0.5 * jnp.exp(-2.0 * log_l)
        scal = jnp.stack([jnp.exp(2.0 * log_s), jnp.exp(2.0 * log_sigma), rate])
        scal = jnp.broadcast_to(jnp.pad(scal, (0, 5))[:, None], (8, 128))
        xt = points_own.T
        pay = jnp.stack([to_half_blocks(xt[:16], xt[16]), to_half_blocks(probes_own.T, targets_own)])
        dma = pltpu.SemaphoreType.DMA
        blocks = pltpu.VMEM((NDEV, 2, 5, 8, 128), f32)
        sol, hyp = pl.pallas_call(
            kernel,
            out_shape=(jax.ShapeDtypeStruct((2, 5, 8, 128), f32), jax.ShapeDtypeStruct((8, 128), f32)),
            in_specs=[pl.BlockSpec(memory_space=pltpu.VMEM)] * 3,
            out_specs=(pl.BlockSpec(memory_space=pltpu.VMEM),) * 2,
            scratch_shapes=[
                pltpu.VMEM((2, 2, NDEV, 5, 8, 128), f32),
                blocks, blocks, blocks, blocks,
                pltpu.VMEM((N, 128), bf16),
                pltpu.VMEM((128, ROWS), bf16),
                pltpu.VMEM((80, N), bf16),
                pltpu.VMEM((72, HALF), f32),
                pltpu.VMEM((2, 2, 5, 8, 128), f32),
                pltpu.VMEM((8, 128), f32),
                pltpu.VMEM((NDEV, 8, 128), f32),
            ] + [pltpu.VMEM((2, PRE, HALF), bf16)] * 3 + [pltpu.VMEM((REST, HALF), bf16)] * 3 + [
                dma((2, NDEV)), dma((2, 2, NDEV)), dma((NDEV,)), dma((NDEV,)),
            ],
            compiler_params=pltpu.CompilerParams(has_side_effects=True, vmem_limit_bytes=67043328),
            name="gp_cg",
        )(pay, scal, jnp.asarray(placements(), bf16))
        v = sol[:, :4].reshape(2, 2, 2, 8, 128).transpose(0, 2, 4, 1, 3).reshape(ROWS, NP)
        u = sol[:, 4, :2].reshape(ROWS)
        return u, v, hyp[:4, 0]

    return jax.shard_map(
        local,
        mesh=mesh,
        in_specs=(P("dp", None), P("dp"), P("dp", None), P(), P(), P()),
        out_specs=(P("dp"), P("dp", None), P()),
        check_vma=False,
    )
```

```python
import math

import jax
import jax.numpy as jnp
import numpy as np
from jax import lax
from jax.experimental import pallas as pl
from jax.experimental.pallas import tpu as pltpu
from jax.sharding import PartitionSpec as P

CG_STEPS = 20
NDEV = 32
ROWS = 512
HALF = 256
NP = 16
DIM = 17
N = NDEV * ROWS
PLANE = 8 * ROWS
ORDER = (0, 1, 3, 2)
WINDOW = (("ahead", 0, 0, 0, 4096), ("line", 1), ("plane", 0), ("ahead", 2, 2, 0, 2048), ("line", 3), ("line", 2),
          ("ahead", 2, 2, 2048, 4096))
BODY = (("rest", 0), ("update", 0), ("apply", 0), ("plane", 1), ("ahead", 3, 0, 0, 2048), ("rest", 1), ("update", 1),
        ("plane", 3), ("apply", 1), ("plane", 2), ("rest", 3), ("update", 3),
        ("apply", 2, (3, 0, 2048, 4096), (1, 1, 0, 1024)), ("rest", 2), ("sent",), ("update", 2), ("rho",),
        ("apply", 0, (1, 1, 1024, 4096)))
LOG2E = math.log2(math.e)
LN2 = math.log(2.0)
f32 = jnp.float32
bf16 = jnp.bfloat16
MESH = pl.DeviceIdType.MESH

TERMS = ((0, 0), (0, 1), (0, 2), (1, 0), (1, 1), (2, 0))


def placements():
    col, row, right, left = (np.zeros((72, 128), np.float32) for _ in range(4))
    j = 0
    for a, b in TERMS:
        for d in range(DIM):
            col[24 * a + d, j] = row[24 * b + d, j] = 1.0
            j += 1
    for t in range(3):
        col[24 * t + 17, j] = row[18, j] = 1.0
        j += 1
    for t in range(3):
        col[18, j] = row[24 * t + 17, j] = 1.0
        j += 1
    j = 0
    for t in range(3):
        for d in range(NP):
            right[d, j] = left[24 * t + d, j] = 1.0
            j += 1
    for a, b in TERMS:
        right[24 * a + NP, j] = left[24 * b + NP, j] = 1.0
        j += 1
    return np.stack([col, row, right, left])


def dot(a, b):
    return lax.dot_general(a, b, (((1,), (0,)), ((), ())), preferred_element_type=f32)


def dot_t(a, b):
    return lax.dot_general(a, b, (((0,), (0,)), ((), ())), preferred_element_type=f32)


def parts(x):
    h = x.astype(bf16).astype(f32)
    r = x - h
    m = r.astype(bf16).astype(f32)
    return h, m, r - m


def wide(v):
    first = lax.broadcasted_iota(jnp.int32, (8, 128), 0) == 0
    last = [jnp.where(first, v[8] if t == 0 else pltpu.roll(v[8], 8 - t, 0), 0.0) for t in range(4)]
    return jnp.concatenate([jnp.concatenate([v[t], v[4 + t], last[t]], axis=0) for t in range(4)], axis=1)


def narrow(q):
    row = lax.broadcasted_iota(jnp.int32, (8, 128), 0)
    last = jnp.zeros((8, 128), f32)
    for t in range(4):
        y = q[16:24, t * 128:(t + 1) * 128]
        last = jnp.where(row == t, y if t == 0 else pltpu.roll(y, t, 0), last)
    return jnp.stack([q[8 * g:8 * g + 8, t * 128:(t + 1) * 128] for g in (0, 1) for t in range(4)] + [last])


def kernel(pay_ref, scal_ref, place_ref, sol_ref, hyp_ref,
           gq, rall, pyall, uyall, pown, uown, xk, xi, pp, acc, qown, tsum, tall,
           h0, m0, l0, h1, m1, l1, h2, m2, l2, send, recv, t_send, t_recv):
    me = lax.axis_index("dp")
    core = lax.rem(me, 2)
    sib = me + 1 - 2 * core
    out_var = scal_ref[0:1, 0:1]
    noise_var = scal_ref[1:2, 0:1]
    rate = scal_ref[2:3, 0:1]
    slots = ((h0, m0, l0), (h1, m1, l1), (h2, m2, l2))

    def flip(i, bit):
        return i + bit - 2 * bit * lax.rem(i // bit, 2)

    def shift_z(i, k):
        return lax.rem(i // 8 + k, 4) * 8 + lax.rem(i, 8)

    def plane_of(k):
        return lax.rem(me // 8 + k, 4)

    nbrs = (flip(me, 2), flip(me, 4), flip(flip(me, 2), 4))
    sib_plane = (sib, flip(sib, 2), flip(sib, 4), flip(flip(sib, 2), 4))

    class Gather:
        def __init__(self, slot, src, into=None):
            self.slot, self.src = slot, src
            self.into = into or (lambda block: gq.at[slot, block])

        def copy(self, block, src, to):
            return pltpu.make_async_remote_copy(
                src_ref=src, dst_ref=self.into(block), send_sem=send.at[0],
                recv_sem=recv.at[self.slot, block], device_id=(to,), device_id_type=MESH)

        def arrived(self, block):
            self.copy(block, self.src, sib).wait_recv()
            return self.into(block)

        def own(self):
            for dz in (1, 3, 2):
                self.copy(me, self.src, shift_z(me, dz)).start()
            for t in nbrs:
                self.copy(me, self.src, t).start()
            self.copy(me, self.src, sib).start()

        def line(self, dz):
            b = shift_z(me, dz)
            src = self.arrived(b)
            for t in nbrs:
                self.copy(b, src, t).start()
            self.copy(b, src, sib).start()

        def plane(self, dz):
            for t in nbrs:
                b = shift_z(t, dz)
                self.copy(b, self.arrived(b), sib).start()

        def rest(self, dz):
            for t in sib_plane:
                self.arrived(shift_z(t, dz))

        def sent(self):
            many = gq.at[0, pl.ds(0, NDEV - 1)]
            pltpu.make_async_remote_copy(src_ref=many, dst_ref=many, send_sem=send.at[0], recv_sem=recv.at[self.slot, me],
                                         device_id=(sib,), device_id_type=MESH).wait_send()

    def split_to(e, bufs, idx):
        hr, mr, lr = bufs
        hr[idx] = e.astype(bf16)
        r = e - hr[idx].astype(f32)
        mr[idx] = r.astype(bf16)
        lr[idx] = (r - mr[idx].astype(f32)).astype(bf16)

    def entries(s, bufs, c, sub=64):
        for r in range(0, s.shape[0], sub):
            for h in (0, 1):
                e = jnp.exp2(jnp.minimum(s[r:r + sub, h * HALF:(h + 1) * HALF], 0.0))
                split_to(e, bufs, (h, pl.ds(c + r, sub), slice(None)))

    def ahead(dz, slot, lo, hi, rows=2048):
        base = plane_of(dz) * PLANE

        def body(i, c):
            c0 = pl.multiple_of(i * rows, rows)
            for j in range(0, rows, 256):
                entries(dot(xk[pl.ds(base + c0 + j, 256), :], xi[...]), slots[slot], c0 + j)
            return c
        lax.fori_loop(lo // rows, hi // rows, body, 0)

    def apply(slot, new):
        todo = [(plane_of(dz) * PLANE, slots[to], c) for dz, to, lo, hi in new for c in range(lo, hi, 256)]
        for h in (0, 1):
            mine = todo[h * len(todo) // 2:(h + 1) * len(todo) // 2]
            subs = max(1, len(mine))
            cuts = [256 * (PLANE // 256 * j // subs) for j in range(subs + 1)]
            total = None
            for j in range(subs):
                if mine:
                    base, bufs, col = mine[j]
                    s = dot(xk[pl.ds(base + col, 256), :], xi[...])
                kk, w = cuts[j], cuts[j + 1] - cuts[j]
                p = jnp.concatenate([pp[:, kk:kk + w], jnp.zeros((48, w), bf16)], axis=0)
                for ref in slots[slot]:
                    d = dot(p, ref[h, kk:kk + w, :])
                    total = d if total is None else total + d
                if mine:
                    entries(s, bufs, col)
            acc[:, h * HALF:(h + 1) * HALF] += total[0:72]

    row24 = lax.broadcasted_iota(jnp.int32, (24, ROWS), 0)

    def augmented(v, scale):
        w = wide(v)
        norm = -rate * jnp.sum(w * w, axis=0, keepdims=True)
        return jnp.where(row24 == 17, norm, jnp.where(row24 == 18, 1.0, w * scale))

    def stack(x):
        return jnp.concatenate(parts(x), axis=0).astype(bf16)

    zero9 = jnp.zeros((9, 8, 128), f32)
    rall[me] = pay_ref[0]
    gq[2, me] = pay_ref[1]
    xs = Gather(0, pay_ref.at[0], lambda b: rall.at[b])
    bs = Gather(2, pay_ref.at[1])
    xs.own()
    xi[...] = dot_t(place_ref[1], stack(augmented(pay_ref[0], 2.0 * rate))).astype(bf16)
    xs.plane(0)
    for dz in (1, 3, 2):
        xs.line(dz)
    for dz in (1, 3, 2):
        xs.plane(dz)
    for dz in ORDER:
        xs.rest(dz)
    xs.sent()

    def pack_points(b, c):
        x = stack(augmented(rall[b], 1.0))
        xk[pl.ds(pl.multiple_of(b * ROWS, ROWS), ROWS), :] = dot_t(x, place_ref[0]).astype(bf16)
        rall[b] = zero9
        pyall[b] = jnp.zeros((8, 128), f32)
        uyall[b] = jnp.zeros((8, 128), f32)
        return c

    bs.own()
    lax.fori_loop(0, NDEV, pack_points, 0)
    pown[...] = zero9
    uown[...] = zero9
    bs.plane(0)
    for dz in (1, 3, 2):
        bs.line(dz)
    for j in (0, 1, 2):
        ahead(ORDER[j], j, 0, PLANE)

    def column_sums(x):
        both = jnp.concatenate([x[0] + x[1] + (x[2] + x[3]), x[4] + x[5] + (x[6] + x[7]), x[8]], axis=0)
        s = jnp.sum(both, axis=1, keepdims=True)
        y = s[16:17] + s[17:18] + (s[18:19] + s[19:20])
        return jnp.concatenate([s[0:16], jnp.broadcast_to(y, (8, 1))], axis=0)

    def spread(s):
        a, b, y = (jnp.broadcast_to(s[j:j + 8], (8, 128)) for j in (0, 8, 16))
        return jnp.stack([a] * 4 + [b] * 4 + [y])


    lane_of_row = lax.broadcasted_iota(jnp.int32, (24, 128), 1) == lax.broadcasted_iota(jnp.int32, (24, 128), 0)

    def share(slot, values):
        row = jnp.sum(jnp.where(lane_of_row, values, 0.0), axis=0, keepdims=True)
        tsum[slot, 0:1] = row
        tall[slot, me, 0:1] = row
        for d in range(1, NDEV):
            pltpu.make_async_remote_copy(src_ref=tsum.at[slot, 0:1], dst_ref=tall.at[slot, me, 0:1], send_sem=t_send.at[0],
                                         recv_sem=t_recv.at[slot], device_id=(lax.rem(me + d, NDEV),),
                                         device_id_type=MESH).start()

    def shared(slot):
        many = tall.at[slot, pl.ds(0, NDEV - 1), 0:1]
        cp = pltpu.make_async_remote_copy(src_ref=many, dst_ref=many, send_sem=t_send.at[0], recv_sem=t_recv.at[slot],
                                          device_id=(sib,), device_id_type=MESH)
        cp.wait_send()
        cp.wait_recv()
        t = [tall[slot, b, 0:1] for b in range(NDEV)]
        while len(t) > 1:
            t = [t[j] + t[j + 1] for j in range(0, len(t), 2)]
        return jnp.sum(jnp.where(lane_of_row, t[0], 0.0), axis=1, keepdims=True)

    def last_column(b, r, alpha, beta):
        p = r + beta[8] * pyall[b]
        pyall[b] = p
        uyall[b] = uyall[b] + alpha[8] * p

    def step(i, carry):
        alpha, beta, rho = carry
        slot = lax.rem(i, 2)
        before = lax.rem(i + 1, 2) + 1 - (i + NDEV - 1) // NDEV
        g = Gather(before, qown.at[before])
        acc[...] = jnp.zeros_like(acc)

        def update(dz, total):
            for j in range(8):
                b = plane_of(dz) * 8 + j
                old = rall[b]
                last_column(b, old[8], alpha, beta)
                r = old - alpha * gq[before, b]
                rall[b] = r
                a, m, l = parts(wide(r))
                both = jnp.concatenate([m, a, l, jnp.zeros((8, ROWS), f32)], axis=0)
                pp[:, j * ROWS:(j + 1) * ROWS] = both.astype(bf16)
                total = total + r * r
            return total

        total = zero9
        for op, *arg in BODY:
            if op == "update":
                total = update(arg[0], total)
            elif op == "rho":
                new = spread(column_sums(total))
                beta = new / rho
            elif op == "apply":
                apply(arg[0], [(ORDER[n[0]],) + n[1:] for n in arg[1:]])
            elif op == "ahead":
                ahead(ORDER[arg[0]], *arg[1:])
            else:
                getattr(g, op)(*arg)

        r = rall[me]
        q = out_var * narrow(acc[0:24, :] + acc[24:48, :] + acc[48:72, :]) + noise_var * r + beta * gq[before, me]
        p = r + beta * pown[...]
        pown[...] = p
        gq[slot, me] = q
        qown[slot] = q
        share(slot, column_sums(p * q))

        @pl.when(i < CG_STEPS - 1)
        def pass_on():
            gn = Gather(slot, qown.at[slot])
            gn.own()
            for op, *arg in WINDOW:
                if op == "ahead":
                    ahead(ORDER[arg[0]], *arg[1:])
                else:
                    getattr(gn, op)(*arg)

        t = shared(slot)
        alpha = new / spread(t)
        uown[...] += alpha * p
        return alpha, beta, new
    alpha, beta, _ = lax.fori_loop(0, CG_STEPS, step, (zero9 - 1.0, zero9, zero9 + jnp.inf))

    def finish(b, c):
        last_column(b, rall[b, 8], alpha, beta)
        return c
    lax.fori_loop(0, NDEV, finish, 0)

    is_y = lax.broadcasted_iota(jnp.int32, (9, 8, 128), 0) == 8
    u = uown[...]
    z = gq[2, me]
    sol_ref[...] = u
    left = jnp.where(is_y, u, u * (-1.0 / NP))
    own_sum = left * jnp.where(is_y, u, z)
    fit_sum = jnp.where(is_y, u * z, 0.0)
    ai = dot_t(place_ref[3], stack(wide(left))).astype(bf16)
    pp[0:64, 0:ROWS] = ai[0:64]

    def pair_sums(b, carry):
        a_s, a_l = carry
        right = jnp.concatenate([gq[2, b][0:8], uyall[b][None]], axis=0)
        ck = dot_t(stack(wide(right)), place_ref[2]).astype(bf16)
        for h in (0, 1):
            k0 = pl.multiple_of(b * ROWS + h * HALF, HALF)
            s = dot(xk[pl.ds(k0, HALF), :], xi[...])
            g = dot(ck[h * HALF:(h + 1) * HALF, 0:64], pp[0:64, 0:ROWS])
            for r in range(0, HALF, 8):
                sr = jnp.minimum(s[r:r + 8], 0.0)
                t = jnp.exp2(sr) * g[r:r + 8]
                a_s = a_s + t
                a_l = a_l + t * sr
        return a_s, a_l
    zrow = jnp.zeros((8, ROWS), f32)
    a_s, a_l = lax.fori_loop(0, NDEV, pair_sums, (zrow, zrow))

    def total(x):
        return jnp.sum(jnp.sum(x, axis=1, keepdims=True), axis=0, keepdims=True)

    def total5(x):
        return total(sum(x[j] for j in range(9)))
    g_l = out_var * (-LN2) * total(a_l)
    g_s = out_var * total(a_s)
    g_n = noise_var * total5(own_sum)
    fit = 0.5 * total5(fit_sum)
    r24 = lax.broadcasted_iota(jnp.int32, (24, 1), 0)
    share(0, jnp.where(r24 == 0, g_l, jnp.where(r24 == 1, g_s, jnp.where(r24 == 2, g_n, jnp.where(r24 == 3, fit, 0.0)))) / N)
    hyp_ref[...] = jnp.broadcast_to(shared(0)[0:8], (8, 128))


def to_block(main, last):
    m = main.reshape(2, 8, 4, 128).transpose(0, 2, 1, 3).reshape(8, 8, 128)
    return jnp.concatenate([m, jnp.pad(last.reshape(1, 4, 128), ((0, 0), (0, 4), (0, 0)))], axis=0)


def solution(mesh):
    def local(points_own, targets_own, probes_own, log_l, log_s, log_sigma):
        rate = LOG2E * 0.5 * jnp.exp(-2.0 * log_l)
        scal = jnp.stack([jnp.exp(2.0 * log_s), jnp.exp(2.0 * log_sigma), rate])
        scal = jnp.broadcast_to(jnp.pad(scal, (0, 5))[:, None], (8, 128))
        xt = points_own.T
        pay = jnp.stack([to_block(xt[:16], xt[16]), to_block(probes_own.T, targets_own)])
        dma = pltpu.SemaphoreType.DMA
        blocks = pltpu.VMEM((NDEV, 2, 5, 8, 128), f32)
        sol, hyp = pl.pallas_call(
            kernel,
            out_shape=(jax.ShapeDtypeStruct((9, 8, 128), f32), jax.ShapeDtypeStruct((8, 128), f32)),
            in_specs=[pl.BlockSpec(memory_space=pltpu.VMEM)] * 3,
            out_specs=(pl.BlockSpec(memory_space=pltpu.VMEM),) * 2,
            scratch_shapes=[
                pltpu.VMEM((3, NDEV, 9, 8, 128), f32),
                pltpu.VMEM((NDEV, 9, 8, 128), f32),
                pltpu.VMEM((NDEV, 8, 128), f32),
                pltpu.VMEM((NDEV, 8, 128), f32),
                pltpu.VMEM((9, 8, 128), f32),
                pltpu.VMEM((9, 8, 128), f32),
                pltpu.VMEM((N, 128), bf16),
                pltpu.VMEM((128, ROWS), bf16),
                pltpu.VMEM((80, PLANE), bf16),
                pltpu.VMEM((72, ROWS), f32),
                pltpu.VMEM((3, 9, 8, 128), f32),
                pltpu.VMEM((2, 8, 128), f32),
                pltpu.VMEM((2, NDEV, 8, 128), f32),
            ] + [pltpu.VMEM((2, PLANE, HALF), bf16)] * 9 + [
                dma((1,)), dma((3, NDEV)), dma((1,)), dma((2,)),
            ],
            compiler_params=pltpu.CompilerParams(has_side_effects=True, vmem_limit_bytes=67043328),
            name="gp_cg",
        )(pay, scal, jnp.asarray(placements(), bf16))
        v = sol[:8].reshape(2, 4, 8, 128).transpose(1, 3, 0, 2).reshape(ROWS, NP)
        u = sol[8, :4].reshape(ROWS)
        return u, v, hyp[:4, 0]

    return jax.shard_map(
        local,
        mesh=mesh,
        in_specs=(P("dp", None), P("dp"), P("dp", None), P(), P(), P()),
        out_specs=(P("dp"), P("dp", None), P()),
        check_vma=False,
    )
```
